32 devices in a mesh: items: 8 (over z, y), users: 4 (over x, core).
Axes of the slice: x: 2, y: 2, z: 4, core: 2. Of those that a mesh axis runs over, the one named last changes fastest.
Arguments:
- user_emb: bfloat16 [4096, 256], P('users', 'items'), as said below
- item_emb: bfloat16 [262144, 256], P('items'), as said below
- target: int32 [4096], P('users'), may hold values from 0 to 262143
- history: int32 [4096, 32], P('users'), may hold values from 0 to 262143, as said below
Outputs:
- log_rank: float32 [4096], P('users')
- metrics: float32 [2], replicated
The draws below stay inside these ranges and needn't reach their ends.
Inputs may be any that keep to these rules, and one draw needn't show every extreme that they name: history[u, k] lies in [k * 8192, (k + 1) * 8192); a user's history entries are thus distinct. `item_emb`: rows of norm about one. `user_emb`: entries of order one.
All inputs are finite; a program needn't handle non-finite values.
Results may differ from the reference program's by a relative error of at most 0.0003.
Values may be sent and summed in bfloat16 or wider, within the bound.
A program may use at most 64 MiB of HBM per device.

```python
import jax
import jax.numpy as jnp
from jax import lax

D = 256
H = 32
ITEMS = 262144
USERS = 4096


def item_row(base, row):
    return jax.random.normal(jax.random.fold_in(base, row), (D,), jnp.float32) / jnp.sqrt(float(D))


def shared_ints(key):
    target = jax.random.randint(jax.random.fold_in(key, 12), (USERS,), 0, ITEMS).astype(jnp.int32)
    stride = ITEMS // H
    offset = jax.random.randint(jax.random.fold_in(key, 13), (USERS, H), 0, stride).astype(jnp.int32)
    history = offset + (jnp.arange(H, dtype=jnp.int32) * stride)[None, :]
    return (target, history)


def draw_item_emb(key, part):
    base = jax.random.fold_in(key, 11)
    rows = jax.vmap(lambda r: item_row(base, r))(jnp.arange(ITEMS, dtype=jnp.int32))
    return rows.astype(jnp.bfloat16)


def draw_target(key, part):
    return shared_ints(key)[0]


def draw_history(key, part):
    return shared_ints(key)[1]


def draw_user_emb(key, part):
    base = jax.random.fold_in(key, 11)
    target, history = shared_ints(key)
    trow = jax.vmap(lambda r: item_row(base, r))(target)
    hrows = jax.vmap(jax.vmap(lambda r: item_row(base, r)))(history)
    noise = jax.random.normal(jax.random.fold_in(key, 14), (USERS, D), jnp.float32) * 0.6
    query = noise + 4.0 * trow + 2.5 * jnp.sum(hrows, axis=1)
    return query.astype(jnp.bfloat16)


def setup_inputs(seed: int = 0) -> dict:
    key_of = jax.random.split(jax.random.key(seed), 5)
    return {
        "user_emb": draw_user_emb(jax.random.fold_in(key_of[4], 71), 0),
        "item_emb": draw_item_emb(jax.random.fold_in(key_of[4], 71), 0),
        "target": draw_target(jax.random.fold_in(key_of[4], 71), 0),
        "history": draw_history(jax.random.fold_in(key_of[4], 71), 0),
    }


sharpness = 4.0


def reference(user_emb, item_emb, target, history):
    users = user_emb.astype(jnp.float32)
    items = item_emb.astype(jnp.float32)
    tscore = jnp.sum(users * items[target], axis=1)
    blk = min(ITEMS, 8192)
    nblk = ITEMS // blk
    blocks = items.reshape(nblk, blk, D)

    def step(total, rows):
        score = jnp.dot(users, rows.T, preferred_element_type=jnp.float32, precision=lax.Precision.HIGHEST)
        return total + jnp.sum(jax.nn.sigmoid(sharpness * (score - tscore[:, None])), axis=1), None

    total, _ = lax.scan(step, jnp.zeros((USERS,), jnp.float32), blocks)
    hrows = items[history]
    hscore = jnp.einsum("ud,uhd->uh", users, hrows, precision=lax.Precision.HIGHEST)
    seen_sum = jnp.sum(jax.nn.sigmoid(sharpness * (hscore - tscore[:, None])), axis=1)
    seen = jnp.any(history == target[:, None], axis=1)
    above = total - seen_sum - jnp.where(seen, 0.0, 0.5).astype(jnp.float32)
    rank = 1.0 + above
    log_rank = jnp.log(rank)
    hit = jax.nn.sigmoid(10.5 - rank)
    gain = hit / jnp.log2(1.0 + rank)
    metrics = jnp.stack([jnp.sum(hit), jnp.sum(gain)]) / USERS
    return log_rank, metrics
```

```python
import functools

import jax
import jax.numpy as jnp
from jax import lax
from jax.experimental import pallas as pl
from jax.experimental.pallas import tpu as pltpu
from jax.sharding import PartitionSpec as P

MESH = pl.DeviceIdType.MESH
BLOCK = 256
ROWS = 64
DEPTH = 8
TRIP = 8192
LEVELS = 5
TROWS = 256


def exchange(axis, n, me, src, dst, send, recv):
    copies = []
    for off in range(1, n):
        peer = lax.rem(me + off, n)
        copies.append(
            pltpu.make_async_remote_copy(
                src_ref=src,
                dst_ref=dst,
                send_sem=send.at[off - 1],
                recv_sem=recv.at[off - 1],
                device_id={axis: peer},
                device_id_type=MESH,
            )
        )
    for c in copies:
        c.start()
    return copies


def pick(tgt_ref, item_ref, own_ref, sem):
    item_dev = item_ref.shape[0]
    base = lax.axis_index("items") * item_dev
    batch = 16

    def body(i, count):
        for j in range(batch):
            user = i * batch + j
            local = tgt_ref[user] - base
            here = (local >= 0) & (local < item_dev)
            row = pl.multiple_of(local & (item_dev - 8), 8)

            @pl.when(here)
            def _():
                pltpu.make_async_copy(
                    item_ref.at[pl.ds(row, 8), :], own_ref.at[pl.ds(pl.multiple_of(user * 8, 8), 8), :], sem
                ).start()

            count = count + here.astype(jnp.int32)
        return count

    count = lax.fori_loop(0, tgt_ref.shape[0] // batch, body, 0)

    def done(i, carry):
        pltpu.make_async_copy(item_ref.at[pl.ds(0, 8), :], own_ref.at[pl.ds(0, 8), :], sem).wait()
        return carry

    lax.fori_loop(0, count, done, 0)


def kernel(
    n, m, u_hbm, own_hbm, item_ref, tgt_hbm, hist_hbm, log_ref, met_ref,
    u_ref, gath, w, items, own, tgt_ref, hist_ref, hrow,
    tpart, tslots, apart, aslots, mpart, mslots,
    sem_item, sem_in, sem_k, us, ur, ts, tr, as_, ar, ms, mr,
):
    me = lax.axis_index("items")
    grp = lax.axis_index("users")
    dsh, u_dev = u_ref.shape
    item_dev, d = items.shape
    hist = hist_ref.shape[0]
    per_shard = hist // n
    span = item_dev // per_shard
    trip = min(span, TRIP)
    trips = item_dev // trip
    nblk = u_dev // BLOCK
    half = trip // 2
    steps = half // ROWS
    pairs = trips // 2

    f_u = pltpu.make_async_copy(u_hbm, u_ref, sem_in.at[0])
    f_t = pltpu.make_async_copy(tgt_hbm, tgt_ref, sem_in.at[1])
    f_o = pltpu.make_async_copy(own_hbm, own, sem_in.at[2])
    f_h = pltpu.make_async_copy(hist_hbm, hist_ref, sem_in.at[3])
    f_i = pltpu.make_async_copy(item_ref, items, sem_item)
    for f in (f_u, f_t, f_h, f_o, f_i):
        f.start()

    barrier = pltpu.get_barrier_semaphore()
    for off in range(1, n):
        pl.semaphore_signal(barrier, inc=1, device_id={"items": lax.rem(me + off, n)}, device_id_type=MESH)
    for off in range(1, m):
        pl.semaphore_signal(barrier, inc=1, device_id={"users": lax.rem(grp + off, m)}, device_id_type=MESH)
    f_u.wait()
    mine = pl.ds(pl.multiple_of(me * dsh, dsh), dsh)
    keep = pltpu.make_async_copy(u_hbm, gath.at[mine, :], sem_k)
    keep.start()
    pl.semaphore_wait(barrier, n - 1 + m - 1)

    ucopies = []
    for b in range(nblk):
        cols = slice(b * BLOCK, (b + 1) * BLOCK)
        ucopies.append(exchange("items", n, me, u_ref.at[:, cols], gath.at[mine, cols], us.at[b], ur.at[b]))

    f_t.wait()
    f_h.wait()
    keep.wait()
    for k in range(hist):
        hrow[k] = hist_ref[k : k + 1, :]
    f_o.wait()
    f_i.wait()

    lane = lax.broadcasted_iota(jnp.int32, (8, 128), 1)
    sub = lax.broadcasted_iota(jnp.int32, (8, 128), 0)
    zero = jnp.zeros((8, 128), jnp.float32)

    def main(accs, taccs):
        def push(blk):
            at = pl.multiple_of(blk * BLOCK, BLOCK)
            for q in range(2):
                pltpu.matmul_push_rhs(w[:, pl.ds(at, BLOCK)], staging_register=0, mxu_index=q)

        def target_scores(b):
            for c in ucopies[b]:
                c.wait()
            cols = slice(b * BLOCK, (b + 1) * BLOCK)
            w[:, cols] = gath[:, cols] * jnp.bfloat16(2)
            push(b)
            pieces = 1024 // TROWS
            got = [zero, zero]

            def feed(k):
                for q in range(2):
                    at = b * BLOCK * 8 + q * 1024 + k * TROWS
                    pltpu.matmul_acc_lhs(
                        taccs[q][k % 2], own[at : at + TROWS, :], load_staged_rhs=0 if k == 0 else None
                    )

            feed(0)
            feed(1)
            for k in range(pieces):
                for q in range(2):
                    pc = pltpu.matmul_pop(taccs[q][k % 2])
                    for r in range(TROWS // 8):
                        at = slice(8 * r, 8 * r + 8)
                        got[q] = jnp.where(lane == k * (TROWS // 8) + r, pc[at, q * 128 : (q + 1) * 128], got[q])
                if k + 2 < pieces:
                    feed(k + 2)
            for q in range(2):
                tgt = tgt_ref[:, b * BLOCK + q * 128 : b * BLOCK + (q + 1) * 128]
                one = jnp.sum(jnp.where(sub == (tgt & 7), got[q], 0.0), axis=0, keepdims=True)
                local = tgt - me * item_dev
                tpart[b, :, q * 128 : (q + 1) * 128] = jnp.where((local >= 0) & (local < item_dev), one, 0.0)
            tslots[b, me] = tpart[b]
            return exchange("items", n, me, tpart.at[b], tslots.at[b, me], ts.at[b], tr.at[b])

        def tile(base, s, q):
            return items[pl.ds(pl.multiple_of(base + (q * half + s * ROWS), ROWS), ROWS), :]

        def report(b, tot):
            for c in range(2):
                s = jnp.sum(tot[c], axis=0, keepdims=True) - float(per_shard)
                apart[b, :, c * 128 : (c + 1) * 128] = 0.5 * s
            aslots[b, me] = apart[b]
            return exchange("items", n, me, apart.at[b], aslots.at[b, me], as_.at[b], ar.at[b])

        tcopies = [target_scores(0)]
        if nblk > 1:
            tcopies.append(target_scores(1))
        push(0)
        for s in range(DEPTH):
            for q in range(2):
                pltpu.matmul_acc_lhs(accs[q][s], tile(0, s, q), load_staged_rhs=0 if s == 0 else None)

        acopies = []
        for b in range(nblk):
            if b > 0 and b + 1 < nblk:
                tcopies.append(target_scores(b + 1))
            for c in tcopies[b]:
                c.wait()
            tsum = tslots[b, 0]
            for i in range(1, n):
                tsum = tsum + tslots[b, i]
            t = [jnp.broadcast_to(tsum[:, c * 128 : (c + 1) * 128], (8, 128)) for c in range(2)]

            def pair(j, carry, b=b, t=t):
                tot = list(carry)
                for h in range(2):
                    cur = 2 * j + h
                    base = pl.multiple_of(cur * trip, trip)
                    row = me * per_shard + lax.div(cur * trip, span)
                    if h == 0:
                        push(b)
                    bits, place = [], []
                    for c in range(2):
                        at = b * BLOCK + c * 128
                        ids = jnp.broadcast_to(hrow[row, :, at : at + 128], (8, 128))
                        bits.append([(ids & half) != 0] + [(ids & (8 << k)) != 0 for k in range(LEVELS - 1)])
                        here = (ids & 7) == sub
                        if trip != span:
                            here = here & ((ids & ~(trip - 1)) == me * item_dev + cur * trip)
                        place.append(jnp.where(here, (ids & (half - 1)) >> (LEVELS + 2), -1))
                    part, count = [None, None], [0, 0]
                    picks = [[], []]
                    for s in range(steps):
                        xs = [pltpu.matmul_pop(accs[q][s % DEPTH]) for q in range(2)]
                        for i in range(ROWS // 8):
                            for c in range(2):
                                for q in range(2):
                                    tau = jnp.tanh(xs[q][8 * i : 8 * i + 8, c * 128 : (c + 1) * 128] - t[c])
                                    part[c] = tau + 8.0 if count[c] == 0 else part[c] + tau
                                    count[c] += 1
                                    if count[c] == 8:
                                        tot[c] = tot[c] + part[c]
                                        count[c] = 0
                                    lvl, v = 0, tau
                                    while picks[c] and picks[c][-1][0] == lvl:
                                        v = jnp.where(bits[c][lvl], v, picks[c].pop()[1])
                                        lvl += 1
                                    if lvl == LEVELS:
                                        group = (s * ROWS + 8 * i) >> (LEVELS + 2)
                                        tot[c] = tot[c] - jnp.where(place[c] == group, v, 0.0)
                                    else:
                                        picks[c].append((lvl, v))
                        for q in range(2):
                            ahead = s + DEPTH
                            load = None
                            if ahead < steps:
                                lhs = tile(base, ahead, q)
                                if h == 0 and s == 0:
                                    load = 0
                            else:
                                nxt = lax.rem(base + trip, item_dev) if h == 1 else base + trip
                                lhs = tile(pl.multiple_of(nxt, trip), ahead - steps, q)
                                if h == 1 and ahead == steps:
                                    load = 0
                                    if q == 0:
                                        push(b + lax.div(j + 1, pairs) if b + 1 < nblk else b)
                            pltpu.matmul_acc_lhs(accs[q][s % DEPTH], lhs, load_staged_rhs=load)
                return tuple(tot)

            acopies.append(report(b, lax.fori_loop(0, pairs, pair, (zero, zero))))
        for s in range(DEPTH):
            for q in range(2):
                pltpu.matmul_pop(accs[q][s])

        seen = jnp.max(jnp.where(hist_ref[...] == tgt_ref[...], 1.0, 0.0), axis=0, keepdims=True)
        hs = jnp.zeros((1, 128), jnp.float32)
        gs = jnp.zeros((1, 128), jnp.float32)
        for b in range(nblk):
            cols = slice(b * BLOCK, (b + 1) * BLOCK)
            for c in acopies[b]:
                c.wait()
            total = aslots[b, 0]
            for i in range(1, n):
                total = total + aslots[b, i]
            rank = 1.0 + (total - jnp.where(seen[:, cols] > 0.5, 0.0, 0.5))
            log_ref[:, cols] = jnp.log(rank)
            hit = jax.nn.sigmoid(10.5 - rank)
            gain = hit / jnp.log2(1.0 + rank)
            for k in range(BLOCK // 128):
                hs = hs + hit[:, k * 128 : (k + 1) * 128]
                gs = gs + gain[:, k * 128 : (k + 1) * 128]
        mpart[:, :128] = hs
        mpart[:, 128:] = gs
        mslots[grp] = mpart[...]
        copies = exchange("users", m, grp, mpart, mslots.at[grp], ms, mr)
        for c in copies:
            c.wait()
        tot = mslots[0]
        for i in range(1, m):
            tot = tot + mslots[i]
        scale = 1.0 / (u_dev * m)
        met_ref[0] = jnp.sum(tot[:, :128]) * scale
        met_ref[1] = jnp.sum(tot[:, 128:]) * scale

    def acc(q, rows):
        return pltpu.ACC(q)((rows, BLOCK), jnp.float32)

    pl.run_scoped(
        main,
        [[acc(q, ROWS) for _ in range(DEPTH)] for q in range(2)],
        [[acc(q, TROWS) for _ in range(2)] for q in range(2)],
    )


def solution(mesh):
    n, m = mesh.shape["items"], mesh.shape["users"]

    def body(user_emb, item_emb, target, history):
        u_dev, dsh = user_emb.shape
        item_dev, d = item_emb.shape
        hist = history.shape[1]
        nblk = u_dev // BLOCK
        vmem = pl.BlockSpec(memory_space=pltpu.VMEM)
        hbm = pl.BlockSpec(memory_space=pltpu.HBM)
        dma = pltpu.SemaphoreType.DMA
        f32 = jnp.float32
        own = pl.pallas_call(
            pick,
            out_shape=jax.ShapeDtypeStruct((u_dev * 8, d), jnp.bfloat16),
            in_specs=[pl.BlockSpec(memory_space=pltpu.SMEM), hbm],
            out_specs=vmem,
            scratch_shapes=[dma(())],
        )(target, item_emb)
        log_rank, metrics = pl.pallas_call(
            functools.partial(kernel, n, m),
            out_shape=(
                jax.ShapeDtypeStruct((1, u_dev), f32),
                jax.ShapeDtypeStruct((2,), f32),
            ),
            in_specs=[hbm] * 5,
            out_specs=(vmem, pl.BlockSpec(memory_space=pltpu.SMEM)),
            scratch_shapes=[
                pltpu.VMEM((dsh, u_dev), jnp.bfloat16),
                pltpu.VMEM((d, u_dev), jnp.bfloat16),
                pltpu.VMEM((d, u_dev), jnp.bfloat16),
                pltpu.VMEM((item_dev, d), jnp.bfloat16),
                pltpu.VMEM((u_dev * 8, d), jnp.bfloat16),
                pltpu.VMEM((1, u_dev), jnp.int32),
                pltpu.VMEM((hist, u_dev), jnp.int32),
                pltpu.VMEM((hist, 1, u_dev), jnp.int32),
                pltpu.VMEM((nblk, 1, BLOCK), f32),
                pltpu.VMEM((nblk, n, 1, BLOCK), f32),
                pltpu.VMEM((nblk, 1, BLOCK), f32),
                pltpu.VMEM((nblk, n, 1, BLOCK), f32),
                pltpu.VMEM((1, 256), f32),
                pltpu.VMEM((m, 1, 256), f32),
                dma(()),
                dma((4,)),
                dma(()),
                dma((nblk, n - 1)), dma((nblk, n - 1)),
                dma((nblk, n - 1)), dma((nblk, n - 1)),
                dma((nblk, n - 1)), dma((nblk, n - 1)),
                dma((m - 1,)), dma((m - 1,)),
            ],
            compiler_params=pltpu.CompilerParams(
                collective_id=0,
                has_side_effects=True,
                vmem_limit_bytes=60 << 20,
            ),
        )(user_emb.T, own, item_emb, target.reshape(1, u_dev), history.T)
        return log_rank.reshape(u_dev), metrics

    return jax.shard_map(
        body,
        mesh=mesh,
        in_specs=(P("users", "items"), P("items", None), P("users"), P("users", None)),
        out_specs=(P("users"), P()),
        check_vma=False,
    )
```

```python
import functools

import jax
import jax.numpy as jnp
from jax import lax
from jax.experimental import pallas as pl
from jax.experimental.pallas import tpu as pltpu
from jax.sharding import PartitionSpec as P

MESH = pl.DeviceIdType.MESH
BLOCK = 256
ROWS = 64
DEPTH = 8
TRIP = 8192
LEVELS = 5
TROWS = 256


def exchange(axis, n, me, src, dst, send, recv):
    copies = []
    for off in range(1, n):
        peer = lax.rem(me + off, n)
        copies.append(
            pltpu.make_async_remote_copy(
                src_ref=src,
                dst_ref=dst,
                send_sem=send.at[off - 1],
                recv_sem=recv.at[off - 1],
                device_id={axis: peer},
                device_id_type=MESH,
            )
        )
    for c in copies:
        c.start()
    return copies


def pick(tgt_ref, tgt_v, item_ref, own_ref, sem):
    tiles = item_ref.shape[0]
    shift = (tiles * 8).bit_length() - 1
    me = lax.axis_index("items")
    batch = 16

    def body(i, carry):
        for j in range(batch):
            user = i * batch + j
            target = tgt_ref[user]

            @pl.when((target >> shift) == me)
            def _():
                pltpu.make_async_copy(item_ref.at[(target >> 3) & (tiles - 1)], own_ref.at[user], sem).start()

        return carry

    lax.fori_loop(0, tgt_ref.shape[0] // batch, body, 0)
    count = jnp.sum(jnp.where((tgt_v[...] >> shift) == me, 1.0, 0.0)).astype(jnp.int32)

    def done(i, carry):
        pltpu.make_async_copy(item_ref.at[0], own_ref.at[0], sem).wait()
        return carry

    lax.fori_loop(0, count, done, 0)


def finish(log_in, met_in, log_out, met_out):
    log_out[...] = log_in[...]
    for i in range(met_in.shape[0]):
        met_out[i] = met_in[i]


def kernel(
    n, m, u_hbm, own_hbm, item_ref, tgt_hbm, hist_hbm, log_ref, met_ref,
    u_ref, gath, w, items, own, tgt_ref, hist_ref, hrow,
    tpart, tslots, apart, aslots, mpart, mslots,
    sem_item, sem_in, sem_k, us, ur, ts, tr, as_, ar, ms, mr,
):
    me = lax.axis_index("items")
    grp = lax.axis_index("users")
    dsh, u_dev = u_ref.shape
    item_dev, d = items.shape
    hist = hist_ref.shape[0]
    per_shard = hist // n
    span = item_dev // per_shard
    trip = min(span, TRIP)
    trips = item_dev // trip
    nblk = u_dev // BLOCK
    half = trip // 2
    steps = half // ROWS
    pairs = trips // 2

    f_u = pltpu.make_async_copy(u_hbm, u_ref, sem_in.at[0])
    f_t = pltpu.make_async_copy(tgt_hbm, tgt_ref, sem_in.at[1])
    f_o = pltpu.make_async_copy(own_hbm, own, sem_in.at[2])
    f_h = pltpu.make_async_copy(hist_hbm, hist_ref, sem_in.at[3])
    f_i = pltpu.make_async_copy(item_ref, items, sem_item)
    for f in (f_u, f_t, f_h, f_o, f_i):
        f.start()

    barrier = pltpu.get_barrier_semaphore()
    for off in range(1, n):
        pl.semaphore_signal(barrier, inc=1, device_id={"items": lax.rem(me + off, n)}, device_id_type=MESH)
    for off in range(1, m):
        pl.semaphore_signal(barrier, inc=1, device_id={"users": lax.rem(grp + off, m)}, device_id_type=MESH)
    f_u.wait()
    mine = pl.ds(pl.multiple_of(me * dsh, dsh), dsh)
    keep = pltpu.make_async_copy(u_hbm, gath.at[mine, :], sem_k)
    keep.start()
    pl.semaphore_wait(barrier, n - 1 + m - 1)

    ucopies = []
    for b in range(nblk):
        cols = slice(b * BLOCK, (b + 1) * BLOCK)
        ucopies.append(exchange("items", n, me, u_ref.at[:, cols], gath.at[mine, cols], us.at[b], ur.at[b]))

    f_t.wait()
    f_h.wait()
    keep.wait()
    for k in range(hist):
        hrow[k] = hist_ref[k : k + 1, :]
    f_o.wait()

    lane = lax.broadcasted_iota(jnp.int32, (8, 128), 1)
    sub = lax.broadcasted_iota(jnp.int32, (8, 128), 0)
    zero = jnp.zeros((8, 128), jnp.float32)

    def main(accs, taccs):
        def push(blk):
            at = pl.multiple_of(blk * BLOCK, BLOCK)
            for q in range(2):
                pltpu.matmul_push_rhs(w[:, pl.ds(at, BLOCK)], staging_register=0, mxu_index=q)

        def target_scores(b):
            for c in ucopies[b]:
                c.wait()
            cols = slice(b * BLOCK, (b + 1) * BLOCK)
            w[:, cols] = gath[:, cols] * jnp.bfloat16(2)
            push(b)
            pieces = 1024 // TROWS
            got = [zero, zero]

            def feed(k):
                for q in range(2):
                    at = b * BLOCK * 8 + q * 1024 + k * TROWS
                    pltpu.matmul_acc_lhs(
                        taccs[q][k % 2], own[at : at + TROWS, :], load_staged_rhs=0 if k == 0 else None
                    )

            feed(0)
            feed(1)
            for k in range(pieces):
                for q in range(2):
                    pc = pltpu.matmul_pop(taccs[q][k % 2])
                    for r in range(TROWS // 8):
                        at = slice(8 * r, 8 * r + 8)
                        got[q] = jnp.where(lane == k * (TROWS // 8) + r, pc[at, q * 128 : (q + 1) * 128], got[q])
                if k + 2 < pieces:
                    feed(k + 2)
            for q in range(2):
                tgt = tgt_ref[:, b * BLOCK + q * 128 : b * BLOCK + (q + 1) * 128]
                one = jnp.sum(jnp.where(sub == (tgt & 7), got[q], 0.0), axis=0, keepdims=True)
                local = tgt - me * item_dev
                tpart[b, :, q * 128 : (q + 1) * 128] = jnp.where((local >= 0) & (local < item_dev), one, 0.0)
            tslots[b, me] = tpart[b]
            return exchange("items", n, me, tpart.at[b], tslots.at[b, me], ts.at[b], tr.at[b])

        def tile(base, s, q):
            return items[pl.ds(pl.multiple_of(base + (q * half + s * ROWS), ROWS), ROWS), :]

        def report(b, tot):
            for c in range(2):
                s = jnp.sum(tot[c], axis=0, keepdims=True) - float(per_shard)
                apart[b, :, c * 128 : (c + 1) * 128] = 0.5 * s
            aslots[b, me] = apart[b]
            return exchange("items", n, me, apart.at[b], aslots.at[b, me], as_.at[b], ar.at[b])

        tcopies = [target_scores(0)]
        if nblk > 1:
            tcopies.append(target_scores(1))
        f_i.wait()
        push(0)
        for s in range(DEPTH):
            for q in range(2):
                pltpu.matmul_acc_lhs(accs[q][s], tile(0, s, q), load_staged_rhs=0 if s == 0 else None)

        acopies = []
        for b in range(nblk):
            if b > 0 and b + 1 < nblk:
                tcopies.append(target_scores(b + 1))
            for c in tcopies[b]:
                c.wait()
            tsum = tslots[b, 0]
            for i in range(1, n):
                tsum = tsum + tslots[b, i]
            t = [jnp.broadcast_to(tsum[:, c * 128 : (c + 1) * 128], (8, 128)) for c in range(2)]

            def pair(j, carry, b=b, t=t):
                tot = list(carry)
                for h in range(2):
                    cur = 2 * j + h
                    base = pl.multiple_of(cur * trip, trip)
                    row = me * per_shard + lax.div(cur * trip, span)
                    if h == 0:
                        push(b)
                    bits, place = [], []
                    for c in range(2):
                        at = b * BLOCK + c * 128
                        ids = jnp.broadcast_to(hrow[row, :, at : at + 128], (8, 128))
                        bits.append([(ids & half) != 0] + [(ids & (8 << k)) != 0 for k in range(LEVELS - 1)])
                        here = (ids & 7) == sub
                        if trip != span:
                            here = here & ((ids & ~(trip - 1)) == me * item_dev + cur * trip)
                        place.append(jnp.where(here, (ids & (half - 1)) >> (LEVELS + 2), -1))
                    part, count = [None, None], [0, 0]
                    picks = [[], []]
                    for s in range(steps):
                        xs = [pltpu.matmul_pop(accs[q][s % DEPTH]) for q in range(2)]
                        for i in range(ROWS // 8):
                            for c in range(2):
                                for q in range(2):
                                    tau = jnp.tanh(xs[q][8 * i : 8 * i + 8, c * 128 : (c + 1) * 128] - t[c])
                                    part[c] = tau + 8.0 if count[c] == 0 else part[c] + tau
                                    count[c] += 1
                                    if count[c] == 8:
                                        tot[c] = tot[c] + part[c]
                                        count[c] = 0
                                    lvl, v = 0, tau
                                    while picks[c] and picks[c][-1][0] == lvl:
                                        v = jnp.where(bits[c][lvl], v, picks[c].pop()[1])
                                        lvl += 1
                                    if lvl == LEVELS:
                                        group = (s * ROWS + 8 * i) >> (LEVELS + 2)
                                        tot[c] = tot[c] - jnp.where(place[c] == group, v, 0.0)
                                    else:
                                        picks[c].append((lvl, v))
                        for q in range(2):
                            ahead = s + DEPTH
                            load = None
                            if ahead < steps:
                                lhs = tile(base, ahead, q)
                                if h == 0 and s == 0:
                                    load = 0
                            else:
                                nxt = lax.rem(base + trip, item_dev) if h == 1 else base + trip
                                lhs = tile(pl.multiple_of(nxt, trip), ahead - steps, q)
                                if h == 1 and ahead == steps:
                                    load = 0
                                    if q == 0:
                                        push(b + lax.div(j + 1, pairs) if b + 1 < nblk else b)
                            pltpu.matmul_acc_lhs(accs[q][s % DEPTH], lhs, load_staged_rhs=load)
                return tuple(tot)

            acopies.append(report(b, lax.fori_loop(0, pairs, pair, (zero, zero))))
        for s in range(DEPTH):
            for q in range(2):
                pltpu.matmul_pop(accs[q][s])

        seen = jnp.max(jnp.where(hist_ref[...] == tgt_ref[...], 1.0, 0.0), axis=0, keepdims=True)
        hs = jnp.zeros((1, 128), jnp.float32)
        gs = jnp.zeros((1, 128), jnp.float32)
        for b in range(nblk):
            cols = slice(b * BLOCK, (b + 1) * BLOCK)
            for c in acopies[b]:
                c.wait()
            total = aslots[b, 0]
            for i in range(1, n):
                total = total + aslots[b, i]
            rank = 1.0 + (total - jnp.where(seen[:, cols] > 0.5, 0.0, 0.5))
            log_ref[:, cols] = jnp.log(rank)
            hit = jax.nn.sigmoid(10.5 - rank)
            gain = hit / jnp.log2(1.0 + rank)
            for k in range(BLOCK // 128):
                hs = hs + hit[:, k * 128 : (k + 1) * 128]
                gs = gs + gain[:, k * 128 : (k + 1) * 128]
        mpart[:, :128] = hs
        mpart[:, 128:] = gs
        mslots[grp] = mpart[...]
        copies = exchange("users", m, grp, mpart, mslots.at[grp], ms, mr)
        for c in copies:
            c.wait()
        tot = mslots[0]
        for i in range(1, m):
            tot = tot + mslots[i]
        scale = 1.0 / (u_dev * m)
        met_ref[0] = jnp.sum(tot[:, :128]) * scale
        met_ref[1] = jnp.sum(tot[:, 128:]) * scale

    def acc(q, rows):
        return pltpu.ACC(q)((rows, BLOCK), jnp.float32)

    pl.run_scoped(
        main,
        [[acc(q, ROWS) for _ in range(DEPTH)] for q in range(2)],
        [[acc(q, TROWS) for _ in range(2)] for q in range(2)],
    )


def solution(mesh):
    n, m = mesh.shape["items"], mesh.shape["users"]

    def body(user_emb, item_emb, target, history):
        u_dev, dsh = user_emb.shape
        item_dev, d = item_emb.shape
        hist = history.shape[1]
        nblk = u_dev // BLOCK
        vmem = pl.BlockSpec(memory_space=pltpu.VMEM)
        hbm = pl.BlockSpec(memory_space=pltpu.HBM)
        dma = pltpu.SemaphoreType.DMA
        f32 = jnp.float32
        smem = pl.BlockSpec(memory_space=pltpu.SMEM)
        own = pl.pallas_call(
            pick,
            out_shape=jax.ShapeDtypeStruct((u_dev, 8, d), jnp.bfloat16),
            in_specs=[smem, vmem, hbm],
            out_specs=vmem,
            scratch_shapes=[dma(())],
        )(target, target.reshape(1, u_dev), item_emb.reshape(item_dev // 8, 8, d))
        outs = (jax.ShapeDtypeStruct((1, u_dev), f32), jax.ShapeDtypeStruct((2,), f32))
        log_rank, metrics = pl.pallas_call(
            functools.partial(kernel, n, m),
            out_shape=outs,
            in_specs=[hbm] * 5,
            out_specs=(vmem, smem),
            scratch_shapes=[
                pltpu.VMEM((dsh, u_dev), jnp.bfloat16),
                pltpu.VMEM((d, u_dev), jnp.bfloat16),
                pltpu.VMEM((d, u_dev), jnp.bfloat16),
                pltpu.VMEM((item_dev, d), jnp.bfloat16),
                pltpu.VMEM((u_dev * 8, d), jnp.bfloat16),
                pltpu.VMEM((1, u_dev), jnp.int32),
                pltpu.VMEM((hist, u_dev), jnp.int32),
                pltpu.VMEM((hist, 1, u_dev), jnp.int32),
                pltpu.VMEM((nblk, 1, BLOCK), f32),
                pltpu.VMEM((nblk, n, 1, BLOCK), f32),
                pltpu.VMEM((nblk, 1, BLOCK), f32),
                pltpu.VMEM((nblk, n, 1, BLOCK), f32),
                pltpu.VMEM((1, 256), f32),
                pltpu.VMEM((m, 1, 256), f32),
                dma(()),
                dma((4,)),
                dma(()),
                dma((nblk, n - 1)), dma((nblk, n - 1)),
                dma((nblk, n - 1)), dma((nblk, n - 1)),
                dma((nblk, n - 1)), dma((nblk, n - 1)),
                dma((m - 1,)), dma((m - 1,)),
            ],
            compiler_params=pltpu.CompilerParams(
                collective_id=0,
                has_side_effects=True,
                vmem_limit_bytes=60 << 20,
            ),
        )(user_emb.T, own.reshape(u_dev * 8, d), item_emb, target.reshape(1, u_dev), history.T)
        log_rank, metrics = pl.pallas_call(
            finish, out_shape=outs, in_specs=[vmem, smem], out_specs=(vmem, smem)
        )(log_rank, metrics)
        return log_rank.reshape(u_dev), metrics

    return jax.shard_map(
        body,
        mesh=mesh,
        in_specs=(P("users", "items"), P("items", None), P("users"), P("users", None)),
        out_specs=(P("users"), P()),
        check_vma=False,
    )
```
